256 devices in a mesh: group: 16 (over z, core), fsdp: 16 (over y, x).
Axes of the slice: x: 4, y: 4, z: 8, core: 2. Of those that a mesh axis runs over, the one named last changes fastest.
Arguments:
- slow_weights: float32 [8960, 1536], P('fsdp'), may hold values from -3 to 3
- fast_weights: bfloat16 [16, 8960, 1536], P('group', 'fsdp'), may hold values from -6 to 6
- momentum: float32 [8960, 1536], P('fsdp', 'group'), may hold values from -0.6 to 0.6
Outputs:
- slow_next: float32 [8960, 1536], P('fsdp')
- momentum_next: float32 [8960, 1536], P('fsdp', 'group')
- fast_next: bfloat16 [8960, 1536], P('fsdp')
The draws below stay inside these ranges and needn't reach their ends.
All inputs are finite; a program needn't handle non-finite values.
Results may differ from the reference program's by a relative error of at most 0.001.
Values sent between devices are 32-bit elements; how exact they have to be, the bound alone decides.
No kernel may reach another device: no remote copies, remote signals or barrier semaphores. Data moves between devices by JAX's collectives and lax.ppermute only.
A program may use at most 64 MiB of HBM per device.

```python
import jax
import jax.numpy as jnp
from jax import lax

D = 1536
FF = 8960
GROUPS = 16


def slow_field(key):
    slow_key = jax.random.fold_in(key, 11)
    return 0.5 * jax.random.truncated_normal(slow_key, -6.0, 6.0, (FF, D), jnp.float32)


def draw_slow_weights(key, part):
    return slow_field(key)


def draw_fast_weights(key, part):
    slow = slow_field(key)
    drift_key = jax.random.fold_in(key, 23)
    key_row, key_col, key_main, key_common = jax.random.split(drift_key, 4)
    row_position = jnp.arange(FF, dtype=jnp.float32) / max(FF - 1, 1)
    col_position = jnp.arange(D, dtype=jnp.float32) / max(D - 1, 1)
    rise = 3.0
    row_scale = 10.0 ** jax.random.uniform(key_row, (FF,), jnp.float32) * rise ** row_position
    col_scale = 10.0 ** jax.random.uniform(key_col, (D,), jnp.float32) * rise ** col_position
    norm_scale = jnp.sqrt(jnp.mean(row_scale * row_scale) * jnp.mean(col_scale * col_scale))
    scale_field = row_scale[:, None] * col_scale[None, :] / norm_scale
    single = jax.random.truncated_normal(key_main, -4.0, 4.0, (GROUPS, FF, D), jnp.float32)
    shared = jax.random.truncated_normal(key_common, -4.0, 4.0, (FF, D), jnp.float32)
    drift = 0.6 * (single + 0.5 * shared[None, :, :])
    drift = jnp.clip(drift * scale_field[None, :, :], -3.0, 3.0)
    return (slow[None, :, :] + drift).astype(jnp.bfloat16)


def shard_levels(own_key, dims, cuts, least, largest):
    loudness = 1.0
    for position, shards_of in cuts:
        draws = jax.random.uniform(jax.random.fold_in(jax.random.fold_in(own_key, 6), position), (shards_of,), jnp.float32, least / len(cuts), largest / len(cuts))
        loudness = loudness * jnp.repeat(jnp.exp(draws), dims[position] // shards_of).reshape((-1,) + (1,) * (len(dims) - 1 - position))
    return loudness


def bell_draw(stream_key, shape, width, reach, cuts=(), kind=jnp.bfloat16):
    level = shard_levels(stream_key, shape, cuts, -0.22, 0.18) if cuts else 1.0
    drawn = jax.random.normal(stream_key, shape, jnp.float32) * width * level
    return jnp.minimum(jnp.maximum(drawn, -reach), reach).astype(kind)


def setup_inputs(seed: int = 0) -> dict:
    key_list = jax.random.split(jax.random.key(seed), 4)
    slow_weights = draw_slow_weights(jax.random.fold_in(key_list[3], 71), 0)
    fast_weights = draw_fast_weights(jax.random.fold_in(key_list[3], 71), 0)
    momentum = bell_draw(key_list[2], (FF, D), 0.1, 0.6, ((0, 16), (1, 16)), jnp.float32)
    return {"slow_weights": slow_weights, "fast_weights": fast_weights, "momentum": momentum}


outer_decay = 0.9
outer_rate = 0.7
max_rms = 0.05
epsilon = 1e-06

def reference(slow_weights, fast_weights, momentum):

    def accumulate(member, running):
        return running + (slow_weights - fast_weights[member].astype(jnp.float32))
    delta_sum = lax.fori_loop(0, GROUPS, accumulate, jnp.zeros(slow_weights.shape, jnp.float32))
    outer_grad = delta_sum / GROUPS
    mean_square = jnp.sum(outer_grad * outer_grad) / (FF * D)
    clip_factor = jnp.minimum(1.0, max_rms / jnp.sqrt(mean_square + epsilon))
    applied = clip_factor * outer_grad
    momentum_next = outer_decay * momentum + applied
    slow_next = slow_weights - outer_rate * (applied + outer_decay * momentum_next)
    fast_next = slow_next.astype(jnp.bfloat16)
    return (slow_next, momentum_next, fast_next)
```

```python
import functools

import jax
import jax.numpy as jnp
from jax import lax
from jax.experimental import pallas as pl
from jax.experimental.pallas import tpu as pltpu
from jax.sharding import Mesh
from jax.sharding import PartitionSpec as P


D = 1536
FF = 8960
GROUPS = 16
ROWS = FF // 16
CHIPS = 8
BLOCK = 96
PACK = (144, 384)
GROUP_ROWS = (144, 144, 144, 128)
SPLITS = (96, 64, 32)

FSDP = ("fsdp_0", "fsdp_1")
GROUP = ("group_0", "group_1")

outer_decay = 0.9
outer_rate = 0.7
max_rms = 0.05
epsilon = 1e-06

ORDER = (
    (True, 4),
    (False, 3),
    (True, 3),
    (False, 2),
    (True, 2),
    (False, 1),
    (True, 1),
    (True, 0),
)
FIRST = 2

RING = []
for _z in range(CHIPS):
    RING.append((2 * _z, 2 * ((_z + 1) % CHIPS)))
    RING.append((2 * _z + 1, 2 * ((_z - 1) % CHIPS) + 1))


def along(value):
    return lax.ppermute(value, GROUP, RING)


def swap(value):
    return lax.ppermute(value, "group_1", [(0, 1), (1, 0)])


def pairs(value, axis, partner, size):
    return lax.ppermute(value, axis, [(i, partner(i)) for i in range(size)])


def lanes():
    return lax.broadcasted_iota(jnp.int32, (1, 128), 1)


def roll(value, amount):
    amount = amount % 128
    return pltpu.roll(value, amount, 1) if amount else value


def packed(read, k, store):
    lane = lanes()
    off = (BLOCK * k) % 128
    tile = (BLOCK * k) // 128

    def group(i, row, rows):
        start = 144 * i + row
        w = read(start, rows, tile)
        if off > 32:
            w = jnp.where(lane >= off, w, read(start, rows, tile + 1))
        return roll(w, 96 * i - off)

    for row, rows in ((0, 128), (128, 16)):
        parts = [group(i, row, rows) for i in range(3)]
        if row < 128:
            parts.append(group(3, row, rows))
        else:
            parts.append(jnp.zeros((rows, 128), jnp.float32))
        for u, split in enumerate(SPLITS):
            store(row, rows, u, jnp.where(lane < split, parts[u], parts[u + 1]))


def for_blocks(z, core, act):
    for k in range(16):
        chip, half = k // 2, k % 2
        away = lax.rem(jnp.where(core == 0, chip - z, z - chip) + CHIPS, CHIPS)
        is_long = core == half
        place = jnp.where(away == 0, 7, jnp.where(is_long, 8 - 2 * away, 7 - 2 * away))
        wanted = jnp.where(is_long, away <= 4, (away >= 1) & (away <= 3))

        @pl.when(wanted)
        def _(k=k, place=place):
            act(k, place)


def send_kernel(fast, first, rest):
    z = lax.axis_index("group_0")
    core = 1 - lax.axis_index("group_1")

    def read(start, rows, tile):
        return fast[0, start : start + rows, 128 * tile : 128 * tile + 128].astype(jnp.float32)

    def act(k, j):
        @pl.when(j < FIRST)
        def _():
            def store(row, rows, u, value):
                first[j, row : row + rows, 128 * u : 128 * u + 128] = value

            packed(read, k, store)

        @pl.when(j >= FIRST)
        def _():
            def store(row, rows, u, value):
                rest[j - FIRST, row : row + rows, 128 * u : 128 * u + 128] = value

            packed(read, k, store)

    for_blocks(z, core, act)


def own_kernel(slow, fast, out):
    z = lax.axis_index("group_0")
    core = lax.axis_index("group_1")

    def read(start, rows, tile):
        at = (slice(start, start + rows), slice(128 * tile, 128 * tile + 128))
        return 2.0 * slow[at] - fast[(0, *at)].astype(jnp.float32)

    def act(k, j):
        def store(row, rows, u, value):
            out[j, row : row + rows, 128 * u : 128 * u + 128] = value

        packed(read, k, store)

    for_blocks(z, core, act)


def block_indices():
    z = lax.axis_index("group_0")
    core = lax.axis_index("group_1")
    sign = 1 - 2 * core

    def block(step, half):
        return 2 * lax.rem(z + sign * step + CHIPS, CHIPS) + half

    return (
        [block(0, core), block(0, 1 - core)]
        + [block(-d, core) for d in (1, 2, 3, 4)]
        + [block(-d, 1 - core) for d in (1, 2, 3)]
        + [block(d, 1 - core) for d in (1, 2, 3, 4)]
        + [block(d, core) for d in (1, 2, 3)]
    )


def final_kernel(*refs):
    clip, slow = refs[:2]
    grads, moms = refs[2:18], refs[18:34]
    slow_next, fast_next, update = refs[34:]
    factor = clip[0, 0]
    for k, grad, mom in zip(block_indices(), grads, moms, strict=True):
        applied = factor * grad[...]
        update[k] = applied + outer_decay * (outer_decay * mom[...] + applied)
    lane = lanes()
    for i, rows in enumerate(GROUP_ROWS):
        at = slice(144 * i, 144 * i + rows)
        for quad in range(4):
            parts = []
            for b in range(4):
                k = 4 * quad + b
                tile = lambda u: update[k, :rows, 128 * u : 128 * u + 128]
                if i == 0:
                    r = tile(0)
                elif i == 3:
                    r = tile(2)
                else:
                    r = jnp.where(lane >= SPLITS[i - 1], tile(i - 1), tile(i))
                parts.append(roll(r, 96 * b - 96 * i))
            for u, split in enumerate(SPLITS):
                tile = 3 * quad + u
                cols = slice(128 * tile, 128 * tile + 128)
                value = slow[at, cols] - outer_rate * jnp.where(lane < split, parts[u], parts[u + 1])
                slow_next[at, cols] = value
                fast_next[at, cols] = value.astype(jnp.bfloat16)


def call(kernel, out_shape, mib, scratch=(), n_smem=0, n_in=0, cost=0):
    specs = [pl.BlockSpec(memory_space=pltpu.SMEM)] * n_smem
    specs += [pl.BlockSpec(memory_space=pltpu.VMEM)] * (n_in - n_smem)
    return pl.pallas_call(
        kernel,
        out_shape=out_shape,
        in_specs=specs,
        out_specs=jax.tree.map(lambda _: pl.BlockSpec(memory_space=pltpu.VMEM), out_shape),
        scratch_shapes=list(scratch),
        compiler_params=pltpu.CompilerParams(vmem_limit_bytes=mib << 20),
        cost_estimate=pl.CostEstimate(flops=cost, bytes_accessed=4 << 20, transcendentals=0),
    )


def f32(*shape):
    return jax.ShapeDtypeStruct(shape, jnp.float32)


def gather(own):
    other = swap(own)
    a, b, ax, bx = [own], [other], [], []
    for d in range(1, 5):
        a.append(along(a[-1]))
        if d < 4:
            b.append(along(b[-1]))
        ax.append(swap(a[-1]))
        if d < 4:
            bx.append(swap(b[-1]))
    return [own, other] + a[1:] + b[1:] + ax + bx


def total(value):
    value = value + swap(value)
    for axis in FSDP:
        value = value + pairs(value, axis, lambda i: i ^ 1, 4)
        value = value + pairs(value, axis, lambda i: 3 - i, 4)
    for bit in (1, 2, 4):
        value = value + pairs(value, "group_0", lambda i: i ^ bit, CHIPS)
    return value


def on_device(slow_weights, fast_weights, momentum):
    first, rest = call(
        send_kernel, (f32(FIRST, *PACK), f32(8 - FIRST, *PACK)), 12, n_in=1, cost=1 << 20
    )(fast_weights)
    first, rest = swap(first), swap(rest)
    mine = call(own_kernel, f32(8, *PACK), 16, n_in=2, cost=1 << 20)(slow_weights, fast_weights)

    def part(j):
        theirs = first[j] if j < FIRST else rest[j - FIRST]
        return mine[j] - theirs

    long, short = along(part(0)), along(part(1))
    long, short = along(long + part(2)), along(short + part(3))
    long, short = along(long + part(4)), along(short + part(5))
    short = swap(short)
    long = along(long + part(6))
    grad = (long + part(7) + short) / GROUPS

    mom = jnp.pad(momentum, ((0, 16), (0, 0))).reshape(4, 144, BLOCK)
    mom = mom.transpose(1, 0, 2).reshape(PACK)
    moms = gather(mom)

    square = total(jnp.broadcast_to(jnp.sum(grad * grad), (8, 128)))
    grads = gather(grad)

    mean_square = square[:1, :1] / (FF * D)
    clip = jnp.minimum(1.0, max_rms / jnp.sqrt(mean_square + epsilon))

    own = grad.reshape(144, 4, BLOCK).transpose(1, 0, 2).reshape(576, BLOCK)[:ROWS]
    momentum_next = outer_decay * momentum + clip * own

    slow_next, fast_next = call(
        final_kernel,
        (f32(ROWS, D), jax.ShapeDtypeStruct((ROWS, D), jnp.bfloat16)),
        40,
        scratch=(pltpu.VMEM((16, *PACK), jnp.float32),),
        n_smem=1,
        n_in=34,
        cost=1 << 20,
    )(clip, slow_weights, *grads, *moms)
    return slow_next, momentum_next, fast_next


def solution(mesh):
    torus = Mesh(mesh.devices.reshape(8, 2, 4, 4), ("group_0", "group_1", "fsdp_0", "fsdp_1"))
    in_specs = (P(FSDP, None), P(GROUP, FSDP, None), P(FSDP, GROUP))
    out_specs = (P(FSDP, None), P(FSDP, GROUP), P(FSDP, None))
    return jax.shard_map(
        on_device, mesh=torus, in_specs=in_specs, out_specs=out_specs, check_vma=False
    )
```

```python
import jax
import jax.numpy as jnp
from jax import lax
from jax.experimental import pallas as pl
from jax.experimental.pallas import tpu as pltpu
from jax.sharding import Mesh
from jax.sharding import PartitionSpec as P


D = 1536
FF = 8960
GROUPS = 16
ROWS = FF // 16
CHIPS = 8
BLOCK = 96
PACK = (144, 384)
GROUP_ROWS = (144, 144, 144, 128)
SPLITS = (96, 64, 32)

FSDP = ("fsdp_0", "fsdp_1")
GROUP = ("group_0", "group_1")

outer_decay = 0.9
outer_rate = 0.7
max_rms = 0.05
epsilon = 1e-06

FIRST = 2

RING = []
for _z in range(CHIPS):
    RING.append((2 * _z, 2 * ((_z + 1) % CHIPS)))
    RING.append((2 * _z + 1, 2 * ((_z - 1) % CHIPS) + 1))


def along(value):
    return lax.ppermute(value, GROUP, RING)


def swap(value):
    return lax.ppermute(value, "group_1", [(0, 1), (1, 0)])


def pairs(value, axis, partner, size):
    return lax.ppermute(value, axis, [(i, partner(i)) for i in range(size)])


def lanes():
    return lax.broadcasted_iota(jnp.int32, (1, 128), 1)


def roll(value, amount):
    amount = amount % 128
    return pltpu.roll(value, amount, 1) if amount else value


def packed(read, k, store):
    lane = lanes()
    off = (BLOCK * k) % 128
    tile = (BLOCK * k) // 128

    def group(i, row, rows):
        start = 144 * i + row
        w = read(start, rows, tile)
        if off > 32:
            w = jnp.where(lane >= off, w, read(start, rows, tile + 1))
        return roll(w, 96 * i - off)

    for row, rows in ((0, 128), (128, 16)):
        parts = [group(i, row, rows) for i in range(3)]
        if row < 128:
            parts.append(group(3, row, rows))
        else:
            parts.append(jnp.zeros((rows, 128), jnp.float32))
        for u, split in enumerate(SPLITS):
            store(row, rows, u, jnp.where(lane < split, parts[u], parts[u + 1]))


def unpacked(tile, i, b):
    if i == 0:
        r = tile(0)
    elif i == 3:
        r = tile(2)
    else:
        r = jnp.where(lanes() >= SPLITS[i - 1], tile(i - 1), tile(i))
    return roll(r, 96 * b - 96 * i)


def for_blocks(z, core, act):
    for k in range(16):
        chip, half = k // 2, k % 2
        away = lax.rem(jnp.where(core == 0, chip - z, z - chip) + CHIPS, CHIPS)
        is_long = core == half
        place = jnp.where(away == 0, 7, jnp.where(is_long, 8 - 2 * away, 7 - 2 * away))
        wanted = jnp.where(is_long, away <= 4, (away >= 1) & (away <= 3))

        @pl.when(wanted)
        def _(k=k, place=place):
            act(k, place)


def send_kernel(fast_hbm, mom_hbm, slow_hbm, first, rest, fast, mom, slow, sem):
    loads = []
    for n, (source, target) in enumerate(((fast_hbm, fast), (mom_hbm, mom), (slow_hbm, slow))):
        loads.append(pltpu.make_async_copy(source, target, sem.at[n]))
        loads[-1].start()
    z = lax.axis_index("group_0")
    core = 1 - lax.axis_index("group_1")
    loads[0].wait()

    def read(start, rows, tile):
        return fast[0, start : start + rows, 128 * tile : 128 * tile + 128].astype(jnp.float32)

    def act(k, j):
        @pl.when(j < FIRST)
        def _():
            def store(row, rows, u, value):
                first[j, row : row + rows, 128 * u : 128 * u + 128] = value

            packed(read, k, store)

        @pl.when(j >= FIRST)
        def _():
            def store(row, rows, u, value):
                rest[j - FIRST, row : row + rows, 128 * u : 128 * u + 128] = value

            packed(read, k, store)

    for_blocks(z, core, act)
    for load in loads[1:]:
        load.wait()


def own_kernel(slow, fast, out):
    z = lax.axis_index("group_0")
    core = lax.axis_index("group_1")

    def read(start, rows, tile):
        at = (slice(start, start + rows), slice(128 * tile, 128 * tile + 128))
        return 2.0 * slow[at] - fast[(0, *at)].astype(jnp.float32)

    def act(k, j):
        def store(row, rows, u, value):
            out[j, row : row + rows, 128 * u : 128 * u + 128] = value

        packed(read, k, store)

    for_blocks(z, core, act)


def mom_kernel(mom_t, out, wide):
    wide[:, :BLOCK] = mom_t[...].T

    def store(row, rows, u, value):
        out[row : row + rows, 128 * u : 128 * u + 128] = value

    packed(lambda start, rows, tile: wide[start : start + rows, :], 0, store)


def own_t_kernel(grad, out, wide):
    for i, rows in enumerate(GROUP_ROWS):
        tile = lambda u: grad[:rows, 128 * u : 128 * u + 128]
        wide[144 * i : 144 * i + rows, :] = unpacked(tile, i, 0)
    out[...] = wide[:, :BLOCK].T


def start_kernel(j):
    def kernel(mine, theirs, out):
        out[...] = mine[j] - theirs[j]

    return kernel


def step_kernel(j):
    def kernel(arrived, mine, theirs, out):
        out[...] = arrived[...] + (mine[j] - theirs[j - FIRST])

    return kernel


def grad_kernel(long, short, mine, theirs, out, square):
    total = long[...] + short[...] + (mine[7] - theirs[7 - FIRST])
    grad = total / GROUPS
    out[...] = grad
    square[...] = jnp.broadcast_to(jnp.sum(grad * grad), (8, 128))


def add_kernel(a, b, out):
    out[...] = a[...] + b[...]


def stack_kernel(*refs):
    out = refs[-1]
    for i, ref in enumerate(refs[:-1]):
        out[i] = ref[...]


def final_kernel(sq_a, sq_b, slow, mom_t, own_t, *refs):
    (grad, grad_o, g5, g2, x5, x2, mom, mom_o, m7, mx) = refs[:10]
    slow_out, fast_out, mom_out, update, slow_buf, fast_buf, mom_buf, sem = refs[10:]
    mean_square = (sq_a[0:1, :] + sq_b[0:1, :]) / (FF * D)
    factor = jnp.minimum(1.0, max_rms / jnp.sqrt(mean_square + epsilon))
    mom_buf[...] = outer_decay * mom_t[...] + factor[:, :1] * own_t[...]
    copies = [pltpu.make_async_copy(mom_buf, mom_out, sem.at[8])]
    copies[0].start()

    z = lax.axis_index("group_0")
    core = lax.axis_index("group_1")
    sign = 1 - 2 * core

    def block(step, half):
        return 2 * lax.rem(z + sign * step + CHIPS, CHIPS) + half

    def place(k, g, m):
        for u in range(3):
            cols = slice(128 * u, 128 * u + 128)
            applied = factor * g(cols)
            update[k, :, cols] = applied + outer_decay * (outer_decay * m(cols) + applied)

    place(block(0, core), lambda c: grad[:, c], lambda c: mom[:, c])
    place(block(0, 1 - core), lambda c: grad_o[:, c], lambda c: mom_o[:, c])
    for n in range(7):
        d, is_b = ((1, 0), (1, 1), (2, 0), (2, 1), (3, 0), (3, 1), (4, 0))[n]
        own_g, far_g, at = (g5, x5, n) if n < 5 else (g2, x2, n - 5)
        half = 1 - core if is_b else core
        place(block(-d, half), lambda c: own_g[at, :, c], lambda c: m7[n, :, c])
        place(block(d, 1 - half), lambda c: far_g[at, :, c], lambda c: mx[n, :, c])

    lane = lanes()
    for i, rows in enumerate(GROUP_ROWS):
        at = slice(144 * i, 144 * i + rows)
        for quad in range(4):
            parts = []
            for b in range(4):
                k = 4 * quad + b
                parts.append(unpacked(lambda u: update[k, :rows, 128 * u : 128 * u + 128], i, b))
            for u, split in enumerate(SPLITS):
                tile = 3 * quad + u
                cols = slice(128 * tile, 128 * tile + 128)
                value = slow[at, cols] - outer_rate * jnp.where(lane < split, parts[u], parts[u + 1])
                slow_buf[at, cols] = value
                fast_buf[at, cols] = value.astype(jnp.bfloat16)
        for n, (buf, out) in enumerate(((slow_buf, slow_out), (fast_buf, fast_out))):
            where = pl.ds(144 * i, rows)
            copies.append(pltpu.make_async_copy(buf.at[where], out.at[where], sem.at[2 * i + n]))
            copies[-1].start()
    for copy in copies:
        copy.wait()


VMEM = pl.BlockSpec(memory_space=pltpu.VMEM)
ANY = pl.BlockSpec(memory_space=pl.ANY)
HBM = pl.BlockSpec(memory_space=pltpu.HBM)


def call(kernel, out_shape, *args, mib=4, scratch=(), in_space=VMEM, out_space=VMEM, flops=1 << 20):
    return pl.pallas_call(
        kernel,
        out_shape=out_shape,
        in_specs=[in_space] * len(args),
        out_specs=jax.tree.map(lambda _: out_space, out_shape),
        scratch_shapes=list(scratch),
        compiler_params=pltpu.CompilerParams(vmem_limit_bytes=mib << 20),
        cost_estimate=pl.CostEstimate(flops=flops, bytes_accessed=1 << 20, transcendentals=0),
    )(*args)


def f32(*shape):
    return jax.ShapeDtypeStruct(shape, jnp.float32)


def step(slow_weights, fast_weights, momentum):
    block = f32(*PACK)
    tile = f32(8, 128)

    loaded = (jax.ShapeDtypeStruct(fast_weights.shape, jnp.bfloat16), f32(BLOCK, ROWS), f32(ROWS, D))
    first, rest, fast_weights, mom_t, slow_weights = call(
        send_kernel,
        (f32(FIRST, *PACK), f32(8 - FIRST, *PACK), *loaded),
        *(pltpu.with_memory_space_constraint(a, pltpu.HBM) for a in (fast_weights, momentum.T, slow_weights)),
        mib=16,
        in_space=HBM,
        scratch=(pltpu.SemaphoreType.DMA((3,)),),
    )
    first, rest = swap(first), swap(rest)
    mine = call(own_kernel, f32(8, *PACK), slow_weights, fast_weights, mib=16)

    mom = call(mom_kernel, block, mom_t, scratch=(pltpu.VMEM((ROWS, 128), jnp.float32),))
    mom_a1 = along(mom)
    mom_o = swap(mom)
    mom_b1 = along(mom_o)
    mom_a2 = along(mom_a1)
    mom_b2 = along(mom_b1)
    mom_a3 = along(mom_a2)
    mom_b3 = along(mom_b2)
    mom_a4 = along(mom_a3)
    m7 = call(stack_kernel, f32(7, *PACK), mom_a1, mom_b1, mom_a2, mom_b2, mom_a3, mom_b3, mom_a4, mib=8)
    mx = swap(m7)

    def add(arrived, j):
        return call(step_kernel(j), block, arrived, mine, rest, mib=8)

    long = along(call(start_kernel(0), block, mine, first, mib=8))
    short = along(call(start_kernel(1), block, mine, first, mib=8))
    long = along(add(long, 2))
    short = along(add(short, 3))
    long = along(add(long, 4))
    short = along(add(short, 5))
    long = along(add(long, 6))
    short = swap(short)
    grad, square = call(grad_kernel, (block, tile), long, short, mine, rest, mib=8)

    def join(a, b):
        return call(add_kernel, tile, a, b, mib=1)

    square = join(square, swap(square))
    x, y = FSDP[1], FSDP[0]
    square = join(square, pairs(square, x, lambda i: i ^ 1, 4))
    square = join(square, pairs(square, x, lambda i: 3 - i, 4))
    square = join(square, pairs(square, y, lambda i: i ^ 1, 4))
    square = join(square, pairs(square, y, lambda i: 3 - i, 4))
    square = join(square, pairs(square, GROUP[0], lambda i: i ^ 1, CHIPS))
    square = join(square, pairs(square, GROUP[0], lambda i: i ^ 2, CHIPS))
    square_far = pairs(square, GROUP[0], lambda i: i ^ 4, CHIPS)

    grad_a1 = along(grad)
    grad_o = swap(grad)
    grad_b1 = along(grad_o)
    grad_a2 = along(grad_a1)
    grad_b2 = along(grad_b1)
    grad_a3 = along(grad_a2)
    grad_b3 = along(grad_b2)
    grad_a4 = along(grad_a3)
    g5 = call(stack_kernel, f32(5, *PACK), grad_a1, grad_b1, grad_a2, grad_b2, grad_a3, mib=8)
    x5 = swap(g5)
    g2 = call(stack_kernel, f32(2, *PACK), grad_b3, grad_a4)
    x2 = swap(g2)

    own_t = call(own_t_kernel, f32(BLOCK, ROWS), grad, scratch=(pltpu.VMEM((ROWS, 128), jnp.float32),))

    slow_next, fast_next, mom_next = call(
        final_kernel,
        (f32(ROWS, D), jax.ShapeDtypeStruct((ROWS, D), jnp.bfloat16), f32(BLOCK, ROWS)),
        square, square_far, slow_weights, mom_t, own_t,
        grad, grad_o, g5, g2, x5, x2, mom, mom_o, m7, mx,
        mib=40,
        out_space=ANY,
        scratch=(
            pltpu.VMEM((16, *PACK), jnp.float32),
            pltpu.VMEM((ROWS, D), jnp.float32),
            pltpu.VMEM((ROWS, D), jnp.bfloat16),
            pltpu.VMEM((BLOCK, ROWS), jnp.float32),
            pltpu.SemaphoreType.DMA((9,)),
        ),
    )
    return slow_next, mom_next.T, fast_next


def solution(mesh):
    torus = Mesh(mesh.devices.reshape(8, 2, 4, 4), ("group_0", "group_1", "fsdp_0", "fsdp_1"))
    in_specs = (P(FSDP, None), P(GROUP, FSDP, None), P(FSDP, GROUP))
    out_specs = (P(FSDP, None), P(FSDP, GROUP), P(FSDP, None))
    return jax.shard_map(step, mesh=torus, in_specs=in_specs, out_specs=out_specs, check_vma=False)
```

```python
import jax
import jax.numpy as jnp
from jax import lax
from jax.experimental import pallas as pl
from jax.experimental.pallas import tpu as pltpu
from jax.sharding import Mesh
from jax.sharding import PartitionSpec as P


D = 1536
FF = 8960
GROUPS = 16
ROWS = FF // 16
CHIPS = 8
BLOCK = 96
PACK = (144, 384)
GROUP_ROWS = (144, 144, 144, 128)
SPLITS = (96, 64, 32)

FSDP = ("fsdp_0", "fsdp_1")
GROUP = ("group_0", "group_1")

outer_decay = 0.9
outer_rate = 0.7
max_rms = 0.05
epsilon = 1e-06

FIRST = 2

RING = []
for _z in range(CHIPS):
    RING.append((2 * _z, 2 * ((_z + 1) % CHIPS)))
    RING.append((2 * _z + 1, 2 * ((_z - 1) % CHIPS) + 1))


def along(value):
    return lax.ppermute(value, GROUP, RING)


def swap(value):
    return lax.ppermute(value, "group_1", [(0, 1), (1, 0)])


def pairs(value, axis, partner, size):
    return lax.ppermute(value, axis, [(i, partner(i)) for i in range(size)])


def lanes():
    return lax.broadcasted_iota(jnp.int32, (1, 128), 1)


def roll(value, amount):
    amount = amount % 128
    return pltpu.roll(value, amount, 1) if amount else value


def packed(read, k, store):
    lane = lanes()
    off = (BLOCK * k) % 128
    tile = (BLOCK * k) // 128

    def group(i, row, rows):
        start = 144 * i + row
        w = read(start, rows, tile)
        if off > 32:
            w = jnp.where(lane >= off, w, read(start, rows, tile + 1))
        return roll(w, 96 * i - off)

    for row, rows in ((0, 128), (128, 16)):
        parts = [group(i, row, rows) for i in range(3)]
        if row < 128:
            parts.append(group(3, row, rows))
        else:
            parts.append(jnp.zeros((rows, 128), jnp.float32))
        for u, split in enumerate(SPLITS):
            store(row, rows, u, jnp.where(lane < split, parts[u], parts[u + 1]))


def unpacked(tile, i, b):
    if i == 0:
        r = tile(0)
    elif i == 3:
        r = tile(2)
    else:
        r = jnp.where(lanes() >= SPLITS[i - 1], tile(i - 1), tile(i))
    return roll(r, 96 * b - 96 * i)


def for_blocks(z, core, act):
    for k in range(16):
        chip, half = k // 2, k % 2
        away = lax.rem(jnp.where(core == 0, chip - z, z - chip) + CHIPS, CHIPS)
        is_long = core == half
        place = jnp.where(away == 0, 7, jnp.where(is_long, 8 - 2 * away, 7 - 2 * away))
        wanted = jnp.where(is_long, away <= 4, (away >= 1) & (away <= 3))

        @pl.when(wanted)
        def _(k=k, place=place):
            act(k, place)


def send_kernel(fast_hbm, mom_hbm, slow_hbm, first, rest, fast, mom, slow, sem):
    loads = []
    for n, (source, target) in enumerate(((fast_hbm, fast), (mom_hbm, mom), (slow_hbm, slow))):
        loads.append(pltpu.make_async_copy(source, target, sem.at[n]))
        loads[-1].start()
    z = lax.axis_index("group_0")
    core = 1 - lax.axis_index("group_1")
    loads[0].wait()

    def read(start, rows, tile):
        return fast[0, start : start + rows, 128 * tile : 128 * tile + 128].astype(jnp.float32)

    def act(k, j):
        @pl.when(j < FIRST)
        def _():
            def store(row, rows, u, value):
                first[j, row : row + rows, 128 * u : 128 * u + 128] = value

            packed(read, k, store)

        @pl.when(j >= FIRST)
        def _():
            def store(row, rows, u, value):
                rest[j - FIRST, row : row + rows, 128 * u : 128 * u + 128] = value

            packed(read, k, store)

    for_blocks(z, core, act)
    for load in loads[1:]:
        load.wait()


def own_kernel(slow, fast, out):
    z = lax.axis_index("group_0")
    core = lax.axis_index("group_1")

    def read(start, rows, tile):
        at = (slice(start, start + rows), slice(128 * tile, 128 * tile + 128))
        return 2.0 * slow[at] - fast[(0, *at)].astype(jnp.float32)

    def act(k, j):
        def store(row, rows, u, value):
            out[j, row : row + rows, 128 * u : 128 * u + 128] = value

        packed(read, k, store)

    for_blocks(z, core, act)


def mom_kernel(mom_t, out, wide):
    wide[:, :BLOCK] = mom_t[...].T

    def store(row, rows, u, value):
        out[row : row + rows, 128 * u : 128 * u + 128] = value

    packed(lambda start, rows, tile: wide[start : start + rows, :], 0, store)


def own_t_kernel(grad, out, wide):
    for i, rows in enumerate(GROUP_ROWS):
        tile = lambda u: grad[:rows, 128 * u : 128 * u + 128]
        wide[144 * i : 144 * i + rows, :] = unpacked(tile, i, 0)
    out[...] = wide[:, :BLOCK].T


def start_kernel(j):
    def kernel(mine, theirs, out):
        out[...] = mine[j] - theirs[j]

    return kernel


def step_kernel(j):
    def kernel(arrived, mine, theirs, out):
        out[...] = arrived[...] + (mine[j] - theirs[j - FIRST])

    return kernel


def grad_kernel(long, short, mine, theirs, out, square):
    total = long[...] + short[...] + (mine[7] - theirs[7 - FIRST])
    grad = total / GROUPS
    out[...] = grad
    square[...] = jnp.broadcast_to(jnp.sum(grad * grad), (8, 128))


def add_kernel(a, b, out):
    out[...] = a[...] + b[...]


def pair_kernel(a_at, b_at):
    def kernel(a, b, out):
        out[0] = a[...] if a_at is None else a[a_at]
        out[1] = b[...] if b_at is None else b[b_at]

    return kernel


def mom_stack_kernel(a1, b1, a2, b2, with_a3, with_b3, out):
    for n, value in enumerate((a1, b1, a2, b2)):
        out[n] = value[...]
    out[4] = with_a3[1]
    out[5] = with_b3[1]


def grad_stack_kernel(a1, with_b1, a2, with_b2, a3, out):
    for n, value in ((0, a1), (2, a2), (4, a3)):
        out[n] = value[...]
    out[1] = with_b1[0]
    out[3] = with_b2[0]


STACK = ((1, 0), (1, 1), (2, 0), (2, 1), (3, 0), (3, 1), (4, 0))


def place(out, n, own, far):
    z = lax.axis_index("group_0")
    core = lax.axis_index("group_1")
    sign = 1 - 2 * core
    d, is_b = STACK[n]
    half = 1 - core if is_b else core
    out[2 * lax.rem(z - sign * d + CHIPS, CHIPS) + half] = own
    out[2 * lax.rem(z + sign * d + CHIPS, CHIPS) + 1 - half] = far


def place_own(out, own, other):
    z = lax.axis_index("group_0")
    core = lax.axis_index("group_1")
    out[2 * z + core] = own
    out[2 * z + 1 - core] = other


def for_tiles(blocks, i, rows, act):
    lane = lanes()
    for quad in range(4):
        parts = []
        for b in range(4):
            k = 4 * quad + b
            parts.append(unpacked(lambda u: blocks[k, :rows, 128 * u : 128 * u + 128], i, b))
        for u, split in enumerate(SPLITS):
            tile = 3 * quad + u
            act(slice(128 * tile, 128 * tile + 128), jnp.where(lane < split, parts[u], parts[u + 1]))


def base_kernel(slow, mom, mom_o, stack, far, last, far_last, out, blocks):
    place_own(blocks, mom[...], mom_o[...])
    for n in range(6):
        place(blocks, n, stack[n], far[n])
    place(blocks, 6, last[1], far_last[1])
    for i, rows in enumerate(GROUP_ROWS):
        at = slice(144 * i, 144 * i + rows)

        def act(cols, value):
            out[at, cols] = slow[at, cols] - (outer_rate * outer_decay * outer_decay) * value

        for_tiles(blocks, i, rows, act)


def fill_kernel(grad, grad_o, stack, far, last, far_last, out):
    place_own(out, grad[...], grad_o[...])
    for n in range(5):
        place(out, n, stack[n], far[n])
    place(out, 5, last[0], far_last[0])


def final_kernel(sq_a, sq_b, base, mom_t, own_t, last, far_last, blocks, slow_out, fast_out, mom_out, same, *scratch):
    slow_buf, fast_buf, mom_buf, sem = scratch
    del blocks
    place(same, 6, last[...], far_last[...])
    mean_square = (sq_a[0:1, :] + sq_b[0:1, :]) / (FF * D)
    factor = jnp.minimum(1.0, max_rms / jnp.sqrt(mean_square + epsilon))
    rate = (outer_rate * (1.0 + outer_decay)) * factor
    copies = []
    for i, rows in enumerate(GROUP_ROWS):
        at = slice(144 * i, 144 * i + rows)

        def act(cols, value):
            value = base[at, cols] - rate * value
            slow_buf[at, cols] = value
            fast_buf[at, cols] = value.astype(jnp.bfloat16)

        for_tiles(same, i, rows, act)
        for n, (buf, out) in enumerate(((slow_buf, slow_out), (fast_buf, fast_out))):
            where = pl.ds(144 * i, rows)
            copies.append(pltpu.make_async_copy(buf.at[where], out.at[where], sem.at[2 * i + n]))
            copies[-1].start()
    mom_buf[...] = outer_decay * mom_t[...] + factor[:, :1] * own_t[...]
    copies.append(pltpu.make_async_copy(mom_buf, mom_out, sem.at[8]))
    copies[-1].start()
    for copy in copies:
        copy.wait()


VMEM = pl.BlockSpec(memory_space=pltpu.VMEM)
ANY = pl.BlockSpec(memory_space=pl.ANY)
HBM = pl.BlockSpec(memory_space=pltpu.HBM)


def call(kernel, out_shape, *args, mib=4, scratch=(), in_space=VMEM, out_space=VMEM, alias=None):
    return pl.pallas_call(
        kernel,
        out_shape=out_shape,
        in_specs=[in_space] * len(args),
        out_specs=jax.tree.map(lambda _: out_space, out_shape) if out_space is VMEM else out_space,
        input_output_aliases=alias or {},
        scratch_shapes=list(scratch),
        compiler_params=pltpu.CompilerParams(vmem_limit_bytes=mib << 20),
        cost_estimate=pl.CostEstimate(flops=1 << 20, bytes_accessed=1 << 20, transcendentals=0),
    )(*args)


def f32(*shape):
    return jax.ShapeDtypeStruct(shape, jnp.float32)


def step(slow_weights, fast_weights, momentum):
    block = f32(*PACK)
    tile = f32(8, 128)

    loaded = (jax.ShapeDtypeStruct(fast_weights.shape, jnp.bfloat16), f32(BLOCK, ROWS), f32(ROWS, D))
    first, rest, fast_weights, mom_t, slow_weights = call(
        send_kernel,
        (f32(FIRST, *PACK), f32(8 - FIRST, *PACK), *loaded),
        *(pltpu.with_memory_space_constraint(a, pltpu.HBM) for a in (fast_weights, momentum.T, slow_weights)),
        mib=16,
        in_space=HBM,
        scratch=(pltpu.SemaphoreType.DMA((3,)),),
    )
    first, rest = swap(first), swap(rest)
    mine = call(own_kernel, f32(8, *PACK), slow_weights, fast_weights, mib=16)

    mom = call(mom_kernel, block, mom_t, scratch=(pltpu.VMEM((ROWS, 128), jnp.float32),))
    mom_a1 = along(mom)
    mom_o = swap(mom)
    mom_b1 = along(mom_o)
    mom_a2 = along(mom_a1)
    mom_b2 = along(mom_b1)

    def add(arrived, j):
        return call(step_kernel(j), block, arrived, mine, rest, mib=8)

    long = along(call(start_kernel(0), block, mine, first, mib=8))
    short = along(call(start_kernel(1), block, mine, first, mib=8))
    long = along(add(long, 2))
    short = along(add(short, 3))
    long = along(add(long, 4))
    short = along(add(short, 5))
    long = along(add(long, 6))
    short = swap(short)
    grad, square = call(grad_kernel, (block, tile), long, short, mine, rest, mib=8)

    def join(a, b):
        return call(add_kernel, tile, a, b, mib=1)

    square = join(square, swap(square))
    x, y = FSDP[1], FSDP[0]
    square = join(square, pairs(square, x, lambda i: i ^ 1, 4))
    square = join(square, pairs(square, x, lambda i: 3 - i, 4))
    square = join(square, pairs(square, y, lambda i: i ^ 1, 4))
    square = join(square, pairs(square, y, lambda i: 3 - i, 4))
    square = join(square, pairs(square, GROUP[0], lambda i: i ^ 1, CHIPS))
    square = join(square, pairs(square, GROUP[0], lambda i: i ^ 2, CHIPS))
    square_far = pairs(square, GROUP[0], lambda i: i ^ 4, CHIPS)

    two = f32(2, *PACK)
    grad_a1 = along(grad)
    grad_o = swap(grad)
    grad_b1 = along(call(pair_kernel(None, None), two, grad_o, mom_a2))
    grad_a2 = along(grad_a1)
    grad_b2 = along(call(pair_kernel(0, None), two, grad_b1, mom_b2))
    grad_a3 = along(grad_a2)
    grad_b3 = along(call(pair_kernel(0, 1), two, grad_b2, grad_b1))
    grad_a4 = along(grad_a3)

    m6 = call(mom_stack_kernel, f32(6, *PACK), mom_a1, mom_b1, mom_a2, mom_b2, grad_b1, grad_b2, mib=8)
    mx = swap(m6)
    g5 = call(grad_stack_kernel, f32(5, *PACK), grad_a1, grad_b1, grad_a2, grad_b2, grad_a3, mib=8)
    x5 = swap(g5)
    xb = swap(grad_b3)
    xa = swap(grad_a4)

    blocks = f32(16, *PACK)
    base = call(
        base_kernel, f32(ROWS, D), slow_weights, mom, mom_o, m6, mx, grad_b3, xb,
        mib=16, scratch=(pltpu.VMEM(blocks.shape, jnp.float32),),
    )
    grads = call(fill_kernel, blocks, grad, grad_o, g5, x5, grad_b3, xb, mib=16)
    own_t = call(own_t_kernel, f32(BLOCK, ROWS), grad, scratch=(pltpu.VMEM((ROWS, 128), jnp.float32),))

    slow_next, fast_next, mom_next, _ = call(
        final_kernel,
        (f32(ROWS, D), jax.ShapeDtypeStruct((ROWS, D), jnp.bfloat16), f32(BLOCK, ROWS), blocks),
        square, square_far, base, mom_t, own_t, grad_a4, xa, grads,
        mib=20,
        out_space=(ANY, ANY, ANY, VMEM),
        alias={7: 3},
        scratch=(
            pltpu.VMEM((ROWS, D), jnp.float32),
            pltpu.VMEM((ROWS, D), jnp.bfloat16),
            pltpu.VMEM((BLOCK, ROWS), jnp.float32),
            pltpu.SemaphoreType.DMA((9,)),
        ),
    )
    return slow_next, mom_next.T, fast_next


def solution(mesh):
    torus = Mesh(mesh.devices.reshape(8, 2, 4, 4), ("group_0", "group_1", "fsdp_0", "fsdp_1"))
    in_specs = (P(FSDP, None), P(GROUP, FSDP, None), P(FSDP, GROUP))
    out_specs = (P(FSDP, None), P(FSDP, GROUP), P(FSDP, None))
    return jax.shard_map(step, mesh=torus, in_specs=in_specs, out_specs=out_specs, check_vma=False)
```

```python
import jax
import jax.numpy as jnp
from jax import lax
from jax.experimental import pallas as pl
from jax.experimental.pallas import tpu as pltpu
from jax.sharding import Mesh
from jax.sharding import PartitionSpec as P


D = 1536
FF = 8960
GROUPS = 16
ROWS = FF // 16
CHIPS = 8
BLOCK = 96
PACK = (144, 384)
GROUP_ROWS = (144, 144, 144, 128)
SPLITS = (96, 64, 32)

FSDP = ("fsdp_0", "fsdp_1")
GROUP = ("group_0", "group_1")

outer_decay = 0.9
outer_rate = 0.7
max_rms = 0.05
epsilon = 1e-06

FIRST = 2

RING = []
for _z in range(CHIPS):
    RING.append((2 * _z, 2 * ((_z + 1) % CHIPS)))
    RING.append((2 * _z + 1, 2 * ((_z - 1) % CHIPS) + 1))


def along(value):
    return lax.ppermute(value, GROUP, RING)


def swap(value):
    return lax.ppermute(value, "group_1", [(0, 1), (1, 0)])


def pairs(value, axis, partner, size):
    return lax.ppermute(value, axis, [(i, partner(i)) for i in range(size)])


def against(value, step):
    links = [(2 * z + c, 2 * ((z + (step if c else -step)) % CHIPS) + c) for z in range(CHIPS) for c in (0, 1)]
    return lax.ppermute(value, GROUP, links)


def lanes():
    return lax.broadcasted_iota(jnp.int32, (1, 128), 1)


def roll(value, amount):
    amount = amount % 128
    return pltpu.roll(value, amount, 1) if amount else value


def packed(read, k, store):
    lane = lanes()
    off = (BLOCK * k) % 128
    tile = (BLOCK * k) // 128

    def group(i, row, rows):
        start = 144 * i + row
        w = read(start, rows, tile)
        if off > 32:
            w = jnp.where(lane >= off, w, read(start, rows, tile + 1))
        return roll(w, 96 * i - off)

    for row, rows in ((0, 128), (128, 16)):
        parts = [group(i, row, rows) for i in range(3)]
        if row < 128:
            parts.append(group(3, row, rows))
        else:
            parts.append(jnp.zeros((rows, 128), jnp.float32))
        for u, split in enumerate(SPLITS):
            store(row, rows, u, jnp.where(lane < split, parts[u], parts[u + 1]))


def unpacked(tile, i, b):
    if i == 0:
        r = tile(0)
    elif i == 3:
        r = tile(2)
    else:
        r = jnp.where(lanes() >= SPLITS[i - 1], tile(i - 1), tile(i))
    return roll(r, 96 * b - 96 * i)


def for_blocks(z, core, act):
    for k in range(16):
        chip, half = k // 2, k % 2
        away = lax.rem(jnp.where(core == 0, chip - z, z - chip) + CHIPS, CHIPS)
        is_long = core == half
        place = jnp.where(away == 0, 7, jnp.where(is_long, 8 - 2 * away, 7 - 2 * away))
        wanted = jnp.where(is_long, away <= 4, (away >= 1) & (away <= 3))

        @pl.when(wanted)
        def _(k=k, place=place):
            act(k, place)


def send_kernel(fast_hbm, mom_hbm, slow_hbm, first, rest, fast, mom, slow, sem):
    loads = []
    for n, (source, target) in enumerate(((fast_hbm, fast), (mom_hbm, mom), (slow_hbm, slow))):
        loads.append(pltpu.make_async_copy(source, target, sem.at[n]))
        loads[-1].start()
    z = lax.axis_index("group_0")
    core = 1 - lax.axis_index("group_1")
    loads[0].wait()

    def read(start, rows, tile):
        return fast[0, start : start + rows, 128 * tile : 128 * tile + 128].astype(jnp.float32)

    def act(k, j):
        @pl.when(j < FIRST)
        def _():
            def store(row, rows, u, value):
                first[j, row : row + rows, 128 * u : 128 * u + 128] = value

            packed(read, k, store)

        @pl.when(j >= FIRST)
        def _():
            def store(row, rows, u, value):
                rest[j - FIRST, row : row + rows, 128 * u : 128 * u + 128] = value

            packed(read, k, store)

    for_blocks(z, core, act)
    for load in loads[1:]:
        load.wait()


def own_kernel(slow, fast, out):
    z = lax.axis_index("group_0")
    core = lax.axis_index("group_1")

    def read(start, rows, tile):
        at = (slice(start, start + rows), slice(128 * tile, 128 * tile + 128))
        return 2.0 * slow[at] - fast[(0, *at)].astype(jnp.float32)

    def act(k, j):
        def store(row, rows, u, value):
            out[j, row : row + rows, 128 * u : 128 * u + 128] = value

        packed(read, k, store)

    for_blocks(z, core, act)


def mom_kernel(mom_t, out, wide):
    wide[:, :BLOCK] = mom_t[...].T

    def store(row, rows, u, value):
        out[row : row + rows, 128 * u : 128 * u + 128] = value

    packed(lambda start, rows, tile: wide[start : start + rows, :], 0, store)


def own_t_kernel(grad, out, wide):
    for i, rows in enumerate(GROUP_ROWS):
        tile = lambda u: grad[:rows, 128 * u : 128 * u + 128]
        wide[144 * i : 144 * i + rows, :] = unpacked(tile, i, 0)
    out[...] = wide[:, :BLOCK].T


HALVES = (slice(0, 72), slice(72, 144))


def start_kernel(j):
    def kernel(mine, theirs, out):
        out[...] = mine[j] - theirs[j]

    return kernel


def start_halves_kernel(mine, theirs, *outs):
    for rows, out in zip(HALVES, outs):
        out[...] = mine[0, rows] - theirs[0, rows]


def half_kernel(j, rows):
    def kernel(arrived, mine, theirs, out):
        out[...] = arrived[...] + (mine[j, rows] - theirs[j - FIRST, rows])

    return kernel


def step_kernel(j):
    def kernel(arrived, mine, theirs, out):
        out[...] = arrived[...] + (mine[j] - theirs[j - FIRST])

    return kernel


def grad_kernel(long_a, long_b, short, mine, theirs, out, square):
    square_sum = 0.0
    for rows, long in zip(HALVES, (long_a, long_b)):
        total = long[...] + short[rows] + (mine[7, rows] - theirs[7 - FIRST, rows])
        grad = total / GROUPS
        out[rows] = grad
        square_sum += jnp.sum(grad * grad)
    square[...] = jnp.broadcast_to(square_sum, (8, 128))


def add_kernel(a, b, out):
    out[...] = a[...] + b[...]


def stack_kernel(*refs):
    out = refs[-1]
    for n, value in enumerate(refs[:-1]):
        out[n] = value[...]


STACK = ((1, 0), (1, 1), (2, 0), (2, 1), (3, 0), (3, 1), (4, 0))


def place(out, n, own, far):
    z = lax.axis_index("group_0")
    core = lax.axis_index("group_1")
    sign = 1 - 2 * core
    d, is_b = STACK[n]
    half = 1 - core if is_b else core
    out[2 * lax.rem(z - sign * d + CHIPS, CHIPS) + half] = own
    out[2 * lax.rem(z + sign * d + CHIPS, CHIPS) + 1 - half] = far


def place_own(out, own, other):
    z = lax.axis_index("group_0")
    core = lax.axis_index("group_1")
    out[2 * z + core] = own
    out[2 * z + 1 - core] = other


def for_tiles(blocks, i, rows, act):
    lane = lanes()
    for quad in range(4):
        parts = []
        for b in range(4):
            k = 4 * quad + b
            parts.append(unpacked(lambda u: blocks[k, :rows, 128 * u : 128 * u + 128], i, b))
        for u, split in enumerate(SPLITS):
            tile = 3 * quad + u
            act(slice(128 * tile, 128 * tile + 128), jnp.where(lane < split, parts[u], parts[u + 1]))


def base_kernel(slow, mom, mom_o, stack, far, out, blocks):
    place_own(blocks, mom[...], mom_o[...])
    for n in range(7):
        place(blocks, n, stack[n], far[n])
    for i, rows in enumerate(GROUP_ROWS):
        at = slice(144 * i, 144 * i + rows)

        def act(cols, value):
            out[at, cols] = slow[at, cols] - (outer_rate * outer_decay * outer_decay) * value

        for_tiles(blocks, i, rows, act)


def fill_kernel(grad, grad_o, stack, far, last, far_last, out):
    place_own(out, grad[...], grad_o[...])
    for n in range(5):
        place(out, n, stack[n], far[n])
    place(out, 5, last[...], far_last[...])


def final_kernel(sq_a, sq_b, base, mom_t, own_t, last, far_last, blocks, slow_out, fast_out, mom_out, same, *scratch):
    slow_buf, fast_buf, mom_buf, sem = scratch
    del blocks
    place(same, 6, last[...], far_last[...])
    mean_square = (sq_a[0:1, :] + sq_b[0:1, :]) / (FF * D)
    factor = jnp.minimum(1.0, max_rms / jnp.sqrt(mean_square + epsilon))
    rate = (outer_rate * (1.0 + outer_decay)) * factor
    copies = []
    mom_buf[...] = outer_decay * mom_t[...] + factor[:, :1] * own_t[...]
    copies.append(pltpu.make_async_copy(mom_buf, mom_out, sem.at[8]))
    copies[-1].start()
    for i, rows in enumerate(GROUP_ROWS):
        at = slice(144 * i, 144 * i + rows)

        def act(cols, value):
            value = base[at, cols] - rate * value
            slow_buf[at, cols] = value
            fast_buf[at, cols] = value.astype(jnp.bfloat16)

        for_tiles(same, i, rows, act)
        for n, (buf, out) in enumerate(((slow_buf, slow_out), (fast_buf, fast_out))):
            where = pl.ds(144 * i, rows)
            copies.append(pltpu.make_async_copy(buf.at[where], out.at[where], sem.at[2 * i + n]))
            copies[-1].start()
    for copy in copies:
        copy.wait()


VMEM = pl.BlockSpec(memory_space=pltpu.VMEM)
ANY = pl.BlockSpec(memory_space=pl.ANY)
HBM = pl.BlockSpec(memory_space=pltpu.HBM)


def call(kernel, out_shape, *args, mib=4, scratch=(), in_space=VMEM, out_space=VMEM, alias=None):
    return pl.pallas_call(
        kernel,
        out_shape=out_shape,
        in_specs=[in_space] * len(args),
        out_specs=jax.tree.map(lambda _: out_space, out_shape) if out_space is VMEM else out_space,
        input_output_aliases=alias or {},
        scratch_shapes=list(scratch),
        compiler_params=pltpu.CompilerParams(vmem_limit_bytes=mib << 20),
        cost_estimate=pl.CostEstimate(flops=1 << 20, bytes_accessed=1 << 20, transcendentals=0),
    )(*args)


def f32(*shape):
    return jax.ShapeDtypeStruct(shape, jnp.float32)


def step(slow_weights, fast_weights, momentum):
    block = f32(*PACK)
    tile = f32(8, 128)

    loaded = (jax.ShapeDtypeStruct(fast_weights.shape, jnp.bfloat16), f32(BLOCK, ROWS), f32(ROWS, D))
    first, rest, fast_weights, mom_t, slow_weights = call(
        send_kernel,
        (f32(FIRST, *PACK), f32(8 - FIRST, *PACK), *loaded),
        *(pltpu.with_memory_space_constraint(a, pltpu.HBM) for a in (fast_weights, momentum.T, slow_weights)),
        mib=16,
        in_space=HBM,
        scratch=(pltpu.SemaphoreType.DMA((3,)),),
    )
    first, rest = swap(first), swap(rest)
    mine = call(own_kernel, f32(8, *PACK), slow_weights, fast_weights, mib=16)

    mom = call(mom_kernel, block, mom_t, scratch=(pltpu.VMEM((ROWS, 128), jnp.float32),))
    mom_a1 = along(mom)
    mom_o = swap(mom)
    mom_a2 = along(mom_a1)
    mom_a3 = along(mom_a2)
    mom_a4 = along(mom_a3)
    mom_b1 = along(mom_o)
    mom_b2 = along(mom_b1)
    mom_b3 = along(mom_b2)

    def add(arrived, j):
        return call(step_kernel(j), block, arrived, mine, rest, mib=8)

    half = f32(72, PACK[1])
    a, b = call(start_halves_kernel, (half, half), mine, first, mib=8)
    a, b = along(a), along(b)
    short = along(call(start_kernel(1), block, mine, first, mib=8))
    for hop, j in ((2, 2), (3, 4), (4, 6)):
        a = call(half_kernel(j, HALVES[0]), half, a, mine, rest, mib=8)
        a = along(a)
        b = call(half_kernel(j, HALVES[1]), half, b, mine, rest, mib=8)
        b = along(b)
        if hop < 4:
            short = along(add(short, j + 1))
    short = swap(short)
    grad, square = call(grad_kernel, (block, tile), a, b, short, mine, rest, mib=8)

    def join(a, b):
        return call(add_kernel, tile, a, b, mib=1)

    square = join(square, swap(square))
    x, y = FSDP[1], FSDP[0]
    square = join(square, pairs(square, x, lambda i: i ^ 1, 4))
    square = join(square, pairs(square, x, lambda i: 3 - i, 4))
    square = join(square, pairs(square, y, lambda i: i ^ 1, 4))
    square = join(square, pairs(square, y, lambda i: 3 - i, 4))
    square = join(square, against(square, 1))
    square = join(square, against(square, 2))
    square_far = against(square, 4)

    grad_a1 = along(grad)
    grad_o = swap(grad)
    grad_b1 = along(grad_o)
    grad_a2 = along(grad_a1)
    grad_b2 = along(grad_b1)
    grad_a3 = along(grad_a2)
    grad_b3 = along(grad_b2)
    grad_a4 = along(grad_a3)

    m7 = call(stack_kernel, f32(7, *PACK), mom_a1, mom_b1, mom_a2, mom_b2, mom_a3, mom_b3, mom_a4, mib=8)
    mx = swap(m7)
    g5 = call(stack_kernel, f32(5, *PACK), grad_a1, grad_b1, grad_a2, grad_b2, grad_a3, mib=8)
    x5 = swap(g5)
    xb = swap(grad_b3)
    xa = swap(grad_a4)

    blocks = f32(16, *PACK)
    base = call(
        base_kernel, f32(ROWS, D), slow_weights, mom, mom_o, m7, mx,
        mib=16, scratch=(pltpu.VMEM(blocks.shape, jnp.float32),),
    )
    grads = call(fill_kernel, blocks, grad, grad_o, g5, x5, grad_b3, xb, mib=16)
    own_t = call(own_t_kernel, f32(BLOCK, ROWS), grad, scratch=(pltpu.VMEM((ROWS, 128), jnp.float32),))

    slow_next, fast_next, mom_next, _ = call(
        final_kernel,
        (f32(ROWS, D), jax.ShapeDtypeStruct((ROWS, D), jnp.bfloat16), f32(BLOCK, ROWS), blocks),
        square, square_far, base, mom_t, own_t, grad_a4, xa, grads,
        mib=20,
        out_space=(ANY, ANY, ANY, VMEM),
        alias={7: 3},
        scratch=(
            pltpu.VMEM((ROWS, D), jnp.float32),
            pltpu.VMEM((ROWS, D), jnp.bfloat16),
            pltpu.VMEM((BLOCK, ROWS), jnp.float32),
            pltpu.SemaphoreType.DMA((9,)),
        ),
    )
    return slow_next, mom_next.T, fast_next


def solution(mesh):
    torus = Mesh(mesh.devices.reshape(8, 2, 4, 4), ("group_0", "group_1", "fsdp_0", "fsdp_1"))
    in_specs = (P(FSDP, None), P(GROUP, FSDP, None), P(FSDP, GROUP))
    out_specs = (P(FSDP, None), P(FSDP, GROUP), P(FSDP, None))
    return jax.shard_map(step, mesh=torus, in_specs=in_specs, out_specs=out_specs, check_vma=False)
```
